32 devices in a mesh: row: 8 (over y, x, core), col: 4 (over z).
Axes of the slice: x: 2, y: 2, z: 4, core: 2. Of those that a mesh axis runs over, the one named last changes fastest.
Arguments:
- value_proj: float32 [8, 4, 1024, 512], P('row', 'col'), may hold values from -6 to 6
- token_pool: bfloat16 [8, 4, 1536, 1024], P('row', 'col'), may hold values from -6 to 6
- target_pool: bfloat16 [8, 4, 1536, 1024], P('row', 'col'), may hold values from -6 to 6
- batch_ids: int32 [8, 4, 3, 1536], P('row', 'col'), may hold values from 0 to 1535
- frozen_out: bfloat16 [512, 1024], replicated, may hold values from -0.25 to 0.25
- numerators: int32 [3], replicated, may hold values from 4 to 15
Outputs:
- final_proj: float32 [8, 4, 1024, 512], P('row', 'col')
- final_tracker: float32 [8, 4, 1024, 512], P('row', 'col')
The draws below stay inside these ranges and needn't reach their ends.
All inputs are finite; a program needn't handle non-finite values.
Results may differ from the reference program's by a relative error of at most 0.017.
Values sent between devices are 32-bit elements; how exact they have to be, the bound alone decides.
A program may use at most 128 MiB of HBM per device.

```python
import jax
import jax.numpy as jnp
from jax import lax

D = 1024
HD = 512
BATCH = 1536
ITERS = 2
POOL = 1536
N_ROW = 8
N_COL = 4


def plant(drawn, stream_key, low, high):
    longest = drawn.shape.index(max(drawn.shape))
    spots = []
    for shift in (0, 1):
        where = [jax.random.randint(jax.random.fold_in(stream_key, axis), (), 0, length) for axis, length in enumerate(drawn.shape)]
        where[longest] = (where[longest] + shift) % drawn.shape[longest]
        spots.append(tuple(where))
    return drawn.at[spots[0]].set(low).at[spots[1]].set(high)


def steps_of(stream_key, shape, split, least, top_value):
    level, own = 1.0, jax.random.fold_in(stream_key, 6)
    for dim, parts in split:
        draws = jnp.exp(jax.random.uniform(jax.random.fold_in(own, dim), (parts,), jnp.float32, least / len(split), top_value / len(split)))
        level = level * jnp.repeat(draws, shape[dim] // parts).reshape([-1 if axis == dim else 1 for axis in range(len(shape))])
    return level


def normal_values(key, dims, width, reach, pieces=(), held_as=jnp.bfloat16):
    values = width * jax.random.normal(key, dims, jnp.float32)
    if pieces:
        values = values * steps_of(key, dims, pieces, -0.22, 0.18)
    return jnp.clip(values, -reach, reach).astype(held_as)


def setup_inputs(seed: int = 0) -> dict:
    streams_of = jax.random.split(jax.random.key(seed), 7)
    return {
        "value_proj": normal_values(streams_of[0], (N_ROW, N_COL, D, HD), 1.0, 6.0, ((0, 8), (1, 4)), jnp.float32),
        "token_pool": normal_values(streams_of[1], (N_ROW, N_COL, POOL, D), 1.0, 6.0, ((0, 8), (1, 4))),
        "target_pool": normal_values(streams_of[2], (N_ROW, N_COL, POOL, D), 1.0, 6.0, ((0, 8), (1, 4))),
        "batch_ids": plant(jax.random.randint(streams_of[3], (N_ROW, N_COL, ITERS + 1, BATCH), 0, POOL), jax.random.fold_in(streams_of[3], 1), 0, POOL - 1).astype(jnp.int32),
        "frozen_out": normal_values(streams_of[4], (HD, D), HD ** -0.5, 0.25),
        "numerators": jax.random.randint(streams_of[5], (3,), 4, 16).astype(jnp.int32),
    }


step_rate = 0.2


def grad_single(current, pool_rows, target_rows, chosen, frozen_out):
    factor = D ** -0.5
    tokens = pool_rows[chosen]
    targets = target_rows[chosen]
    preact = jnp.dot(tokens, current.astype(jnp.bfloat16), preferred_element_type=jnp.float32) * factor
    sigmoid_pre = jax.nn.sigmoid(preact)
    hidden = (preact * sigmoid_pre).astype(jnp.bfloat16)
    output = jnp.dot(hidden, frozen_out, preferred_element_type=jnp.float32)
    error_term = (output - targets.astype(jnp.float32)).astype(jnp.bfloat16)
    back_hidden = lax.dot_general(error_term, frozen_out, (((1,), (1,)), ((), ())), preferred_element_type=jnp.float32)
    slope = sigmoid_pre * (1.0 + preact * (1.0 - sigmoid_pre))
    back_pre = (back_hidden * slope).astype(jnp.bfloat16)
    return lax.dot_general(tokens, back_pre, (((0,), (0,)), ((), ())), preferred_element_type=jnp.float32) * factor


def all_gradients(current, token_pool, target_pool, batch_ids, frozen_out, which):
    count = N_ROW * N_COL

    def flatten(array):
        return array.reshape((count,) + array.shape[2:])

    def single(items):
        return grad_single(items[0], items[1], items[2], items[3], frozen_out)

    result = lax.map(single, (flatten(current), flatten(token_pool), flatten(target_pool), flatten(batch_ids[:, :, which])))
    return result.reshape(current.shape)


def gossip(field, mix_weights):
    return mix_weights[0] * field + mix_weights[1] * jnp.roll(field, 1, 0) + mix_weights[2] * jnp.roll(field, 1, 1)


def reference(value_proj, token_pool, target_pool, batch_ids, frozen_out, numerators):
    counts = numerators.astype(jnp.float32)
    mix_weights = counts / jnp.sum(counts)
    current = value_proj
    grad_old = all_gradients(current, token_pool, target_pool, batch_ids, frozen_out, 0)
    tracker = grad_old
    for which in range(1, ITERS + 1):
        current_new = gossip(current, mix_weights) - step_rate * tracker
        grad_new = all_gradients(current_new, token_pool, target_pool, batch_ids, frozen_out, which)
        tracker = (gossip(tracker, mix_weights) + grad_new) - grad_old
        current = current_new
        grad_old = grad_new
    return current, tracker
```

```python
import functools
import math

import jax
import jax.numpy as jnp
from jax import lax
from jax.experimental import pallas as pl
from jax.experimental.pallas import tpu as pltpu
from jax.sharding import PartitionSpec as P

MESH = pl.DeviceIdType.MESH
step_rate = 0.2
PIECES = 8
AXES = ("row", "col")


def kernel(sizes, x0_ref, tok_hbm, tgt_hbm, ids_hbm, fo_hbm, num_hbm, outx_ref, outy_ref,
           tok, tgt, ids, fo, num_ref, x0, x1, g0, g1, g2, y1, xb, bp,
           x0_in, g0_in, x1_in, y1_in, local_sem, send_sem, recv_sem):
    pool, width = tok.shape
    features = x0.shape[1]
    factor = width ** (-0.5)
    f32, bf16 = jnp.float32, jnp.bfloat16
    piece = width // PIECES
    right, left = {}, {}
    for axis, n in zip(AXES, sizes):
        me = lax.axis_index(axis)
        right[axis], left[axis] = lax.rem(me + 1, n), lax.rem(me + n - 1, n)

    barrier = pltpu.get_barrier_semaphore()
    for axis in AXES:
        for there in (left, right):
            pl.semaphore_signal(
                barrier, inc=1, device_id={axis: there[axis]}, device_id_type=MESH
            )
    loads = []
    for slot, (source, target) in enumerate(
        (
            (x0_ref, x0), (tok_hbm, tok), (fo_hbm, fo),
            (tgt_hbm, tgt), (ids_hbm, ids), (num_hbm, num_ref),
        )
    ):
        load = pltpu.make_async_copy(source, target, local_sem.at[slot])
        load.start()
        loads.append(load)

    pl.semaphore_wait(barrier, 4)

    def send(source, target, which, slot):
        copy = pltpu.make_async_remote_copy(
            src_ref=source,
            dst_ref=target,
            send_sem=send_sem.at[which, slot],
            recv_sem=recv_sem.at[which, slot],
            device_id={AXES[which]: right[AXES[which]]},
            device_id_type=MESH,
        )
        copy.start()
        return copy

    def send_both(source, target, slot):
        return [send(source, target.at[which], which, slot) for which in (1, 0)]

    x0_copies = send_both(x0_ref, x0_in, 0)

    step = math.gcd(width, 64)

    def by_rows(first, last, body):
        def go(i, carry):
            body(pl.ds(pl.multiple_of(i * step, step), step))
            return carry

        lax.fori_loop(first // step, last // step, go, 0)

    def mixed(own, arrived, rows):
        return w[0] * own[rows, :] + w[1] * arrived[0, rows, :] + w[2] * arrived[1, rows, :]

    block = math.gcd(pool, 256)
    wide = math.gcd(width, 256)

    def gradient(which, out):
        def forward(i, carry):
            rows = pl.ds(pl.multiple_of(i * block, block), block)
            preact = jnp.dot(tok[rows, :], xb[...], preferred_element_type=f32) * factor
            s = jax.nn.sigmoid(preact)
            hidden = (preact * s).astype(bf16)
            output = jnp.dot(hidden, fo[...], preferred_element_type=f32)
            error_term = (output - tgt[rows, :].astype(f32)).astype(bf16)
            back_hidden = lax.dot_general(
                error_term, fo[...], (((1,), (1,)), ((), ())), preferred_element_type=f32
            )
            slope = s * (1.0 + preact * (1.0 - s))
            row_ids = lax.broadcasted_iota(jnp.int32, (block, ids.shape[2]), 0) + i * block
            hits = jnp.where(row_ids == ids[which], 1.0, 0.0)
            times = jnp.sum(hits, axis=1, keepdims=True)
            bp[rows, :] = (back_hidden * slope * times).astype(bf16)
            return carry

        lax.fori_loop(0, pool // block, forward, 0)

        for j in range(width // wide):
            cols = pl.ds(j * wide, wide)
            out[cols, :] = (
                lax.dot_general(
                    tok[:, cols], bp[...], (((0,), (0,)), ((), ())), preferred_element_type=f32
                )
                * factor
            )

    for load in loads:
        load.wait()

    counts = [jnp.full((8, 128), num_ref[i], jnp.int32).astype(f32) for i in range(3)]
    total = counts[0] + counts[1] + counts[2]
    w = [(c / total)[0:1, 0:1] for c in counts]

    def first_round(rows):
        xb[rows, :] = x0[rows, :].astype(bf16)

    by_rows(0, width, first_round)
    gradient(0, g0)
    g0_copies = send_both(g0, g0_in, 1)

    for copy in x0_copies:
        copy.wait()

    def first_move(rows):
        moved = mixed(x0, x0_in, rows) - step_rate * g0[rows, :]
        x1[rows, :] = moved
        xb[rows, :] = moved.astype(bf16)

    by_rows(0, width, first_move)
    x1_copies = send_both(x1, x1_in, 2)
    gradient(1, g1)
    for copy in g0_copies:
        copy.wait()

    def first_track(rows):
        y1[rows, :] = mixed(g0, g0_in, rows) + g1[rows, :] - g0[rows, :]

    by_rows(0, width, first_track)
    y1_copies = []
    for part in range(PIECES):
        rows = pl.ds(part * piece, piece)
        y1_copies.append(
            [send(y1.at[rows], y1_in.at[which, rows], which, 3 + part) for which in (1, 0)]
        )

    for copy in x1_copies:
        copy.wait()

    def second_move(rows):
        moved = mixed(x1, x1_in, rows) - step_rate * y1[rows, :]
        outx_ref[rows, :] = moved
        xb[rows, :] = moved.astype(bf16)

    by_rows(0, width, second_move)
    gradient(2, g2)

    def second_track(rows):
        outy_ref[rows, :] = mixed(y1, y1_in, rows) + g2[rows, :] - g1[rows, :]

    for part in range(PIECES):
        for copy in y1_copies[part]:
            copy.wait()
        by_rows(part * piece, (part + 1) * piece, second_track)


def write_out(x_ref, y_ref, x_hbm, y_hbm, sems):
    copies = []
    for slot, (source, target) in enumerate(((x_ref, x_hbm), (y_ref, y_hbm))):
        copy = pltpu.make_async_copy(source, target, sems.at[slot])
        copy.start()
        copies.append(copy)
    for copy in copies:
        copy.wait()


def solution(mesh):
    sizes = tuple(mesh.shape[axis] for axis in AXES)

    def on_device(value_proj, token_pool, target_pool, batch_ids, frozen_out, numerators):
        width, features = value_proj.shape[2:]
        pool = token_pool.shape[2]
        rounds, batch = batch_ids.shape[2:]
        field = pltpu.VMEM((width, features), jnp.float32)
        arrivals = pltpu.VMEM((2, width, features), jnp.float32)
        in_hbm = pl.BlockSpec(memory_space=pltpu.HBM)
        shape = jax.ShapeDtypeStruct((width, features), jnp.float32)
        final_proj, final_tracker = pl.pallas_call(
            functools.partial(kernel, sizes),
            out_shape=(pltpu.VMEM((width, features), jnp.float32),) * 2,
            in_specs=[in_hbm] * 6,
            out_specs=(pl.BlockSpec(memory_space=pltpu.VMEM),) * 2,
            scratch_shapes=[
                pltpu.VMEM((pool, width), jnp.bfloat16),
                pltpu.VMEM((pool, width), jnp.bfloat16),
                pltpu.VMEM((rounds, 1, batch), jnp.int32),
                pltpu.VMEM((features, width), jnp.bfloat16),
                pltpu.SMEM(numerators.shape, jnp.int32),
                field, field, field, field, field, field,
                pltpu.VMEM((width, features), jnp.bfloat16),
                pltpu.VMEM((pool, features), jnp.bfloat16),
                arrivals, arrivals, arrivals, arrivals,
                pltpu.SemaphoreType.DMA((6,)),
                pltpu.SemaphoreType.DMA((2, 3 + PIECES)),
                pltpu.SemaphoreType.DMA((2, 3 + PIECES)),
            ],
            compiler_params=pltpu.CompilerParams(
                collective_id=0, has_side_effects=True, vmem_limit_bytes=54_000_000
            ),
        )(
            value_proj.reshape(width, features),
            token_pool.reshape(pool, width),
            target_pool.reshape(pool, width),
            batch_ids.reshape(rounds, 1, batch),
            frozen_out,
            numerators,
        )
        final_proj, final_tracker = pl.pallas_call(
            write_out,
            out_shape=(shape, shape),
            in_specs=[pl.BlockSpec(memory_space=pltpu.VMEM)] * 2,
            out_specs=(in_hbm,) * 2,
            scratch_shapes=[pltpu.SemaphoreType.DMA((2,))],
            compiler_params=pltpu.CompilerParams(vmem_limit_bytes=2**20),
        )(final_proj, final_tracker)
        return final_proj[None, None], final_tracker[None, None]

    return jax.shard_map(
        on_device,
        mesh=mesh,
        in_specs=(
            P("row", "col", None, None),
            P("row", "col", None, None),
            P("row", "col", None, None),
            P("row", "col", None, None),
            P(),
            P(),
        ),
        out_specs=(P("row", "col", None, None), P("row", "col", None, None)),
        check_vma=False,
    )
```

```python
import functools
import math

import jax
import jax.numpy as jnp
from jax import lax
from jax.experimental import pallas as pl
from jax.experimental.pallas import tpu as pltpu
from jax.sharding import PartitionSpec as P

MESH = pl.DeviceIdType.MESH
step_rate = 0.2
PIECES = 8
OUT_PIECES = 4
AXES = ("row", "col")


def kernel(sizes, x0_ref, tok_hbm, tgt_hbm, ids_hbm, fo_hbm, num_hbm, outx_ref, outy_ref,
           tok, tgt, ids, fo, num_ref, x0, x1, g0, g1, g2, y1, xb, bp,
           x0_in, g0_in, x1_in, y1_in, local_sem, send_sem, recv_sem):
    pool, width = tok.shape
    features = x0.shape[1]
    factor = width ** (-0.5)
    f32, bf16 = jnp.float32, jnp.bfloat16
    piece = width // PIECES
    right, left = {}, {}
    for axis, n in zip(AXES, sizes):
        me = lax.axis_index(axis)
        right[axis], left[axis] = lax.rem(me + 1, n), lax.rem(me + n - 1, n)

    barrier = pltpu.get_barrier_semaphore()
    for axis in AXES:
        pl.semaphore_signal(
            barrier, inc=1, device_id={axis: left[axis]}, device_id_type=MESH
        )
    pl.semaphore_wait(barrier, len(AXES))

    def send(source, target, which, slot):
        copy = pltpu.make_async_remote_copy(
            src_ref=source,
            dst_ref=target,
            send_sem=send_sem.at[which, slot],
            recv_sem=recv_sem.at[which, slot],
            device_id={AXES[which]: right[AXES[which]]},
            device_id_type=MESH,
        )
        copy.start()
        return copy

    def send_both(source, target, slot):
        return [send(source, target.at[which], which, slot) for which in (1, 0)]

    x0_copies = send_both(x0_ref, x0_in, 0)

    loads = []
    for slot, (source, target) in enumerate(
        (
            (x0_ref, x0), (tok_hbm, tok), (fo_hbm, fo),
            (tgt_hbm, tgt), (ids_hbm, ids), (num_hbm, num_ref),
        )
    ):
        load = pltpu.make_async_copy(source, target, local_sem.at[slot])
        load.start()
        loads.append(load)

    step = math.gcd(width, 64)

    def by_rows(first, last, body):
        def go(i, carry):
            body(pl.ds(pl.multiple_of(i * step, step), step))
            return carry

        lax.fori_loop(first // step, last // step, go, 0)

    def mixed(own, arrived, rows):
        return w[0] * own[rows, :] + w[1] * arrived[0, rows, :] + w[2] * arrived[1, rows, :]

    block = math.gcd(pool, 256)
    wide = math.gcd(width, 256)

    def gradient(which, out):
        def forward(i, carry):
            rows = pl.ds(pl.multiple_of(i * block, block), block)
            preact = jnp.dot(tok[rows, :], xb[...], preferred_element_type=f32) * factor
            s = jax.nn.sigmoid(preact)
            hidden = (preact * s).astype(bf16)
            output = jnp.dot(hidden, fo[...], preferred_element_type=f32)
            error_term = (output - tgt[rows, :].astype(f32)).astype(bf16)
            back_hidden = lax.dot_general(
                error_term, fo[...], (((1,), (1,)), ((), ())), preferred_element_type=f32
            )
            slope = s * (1.0 + preact * (1.0 - s))
            row_ids = lax.broadcasted_iota(jnp.int32, (block, ids.shape[2]), 0) + i * block
            hits = jnp.where(row_ids == ids[which], 1.0, 0.0)
            times = jnp.sum(hits, axis=1, keepdims=True)
            bp[rows, :] = (back_hidden * slope * times).astype(bf16)
            return carry

        lax.fori_loop(0, pool // block, forward, 0)

        for j in range(width // wide):
            cols = pl.ds(j * wide, wide)
            out[cols, :] = (
                lax.dot_general(
                    tok[:, cols], bp[...], (((0,), (0,)), ((), ())), preferred_element_type=f32
                )
                * factor
            )

    for load in loads:
        load.wait()

    counts = [jnp.full((8, 128), num_ref[i], jnp.int32).astype(f32) for i in range(3)]
    total = counts[0] + counts[1] + counts[2]
    w = [(c / total)[0:1, 0:1] for c in counts]

    def first_round(rows):
        xb[rows, :] = x0[rows, :].astype(bf16)

    by_rows(0, width, first_round)
    gradient(0, g0)
    g0_copies = send_both(g0, g0_in, 1)

    for copy in x0_copies:
        copy.wait()

    def first_move(rows):
        moved = mixed(x0, x0_in, rows) - step_rate * g0[rows, :]
        x1[rows, :] = moved
        xb[rows, :] = moved.astype(bf16)

    by_rows(0, width, first_move)
    x1_copies = send_both(x1, x1_in, 2)
    gradient(1, g1)
    for copy in g0_copies:
        copy.wait()

    def first_track(rows):
        y1[rows, :] = mixed(g0, g0_in, rows) + g1[rows, :] - g0[rows, :]

    by_rows(0, width, first_track)
    y1_copies = []
    for part in range(PIECES):
        rows = pl.ds(part * piece, piece)
        y1_copies.append(
            [send(y1.at[rows], y1_in.at[which, rows], which, 3 + part) for which in (1, 0)]
        )

    for copy in x1_copies:
        copy.wait()

    def second_move(rows):
        moved = mixed(x1, x1_in, rows) - step_rate * y1[rows, :]
        outx_ref[rows, :] = moved
        xb[rows, :] = moved.astype(bf16)

    by_rows(0, width, second_move)
    gradient(2, g2)

    def second_track(rows):
        outy_ref[rows, :] = mixed(y1, y1_in, rows) + g2[rows, :] - g1[rows, :]

    for part in range(PIECES):
        for copy in y1_copies[part]:
            copy.wait()
        by_rows(part * piece, (part + 1) * piece, second_track)


def write_out(x_ref, y_ref, x_hbm, y_hbm, sems):
    rows = x_ref.shape[0] // OUT_PIECES
    copies = []
    for part in range(OUT_PIECES):
        here = pl.ds(part * rows, rows)
        for which, (source, target) in enumerate(((x_ref, x_hbm), (y_ref, y_hbm))):
            copy = pltpu.make_async_copy(source.at[here], target.at[here], sems.at[which, part])
            copy.start()
            copies.append(copy)
    for copy in copies:
        copy.wait()


def solution(mesh):
    sizes = tuple(mesh.shape[axis] for axis in AXES)

    def on_device(value_proj, token_pool, target_pool, batch_ids, frozen_out, numerators):
        width, features = value_proj.shape[2:]
        pool = token_pool.shape[2]
        rounds, batch = batch_ids.shape[2:]
        field = pltpu.VMEM((width, features), jnp.float32)
        arrivals = pltpu.VMEM((2, width, features), jnp.float32)
        in_hbm = pl.BlockSpec(memory_space=pltpu.HBM)
        shape = jax.ShapeDtypeStruct((width, features), jnp.float32)
        final_proj, final_tracker = pl.pallas_call(
            functools.partial(kernel, sizes),
            out_shape=(pltpu.VMEM((width, features), jnp.float32),) * 2,
            in_specs=[in_hbm] * 6,
            out_specs=(pl.BlockSpec(memory_space=pltpu.VMEM),) * 2,
            scratch_shapes=[
                pltpu.VMEM((pool, width), jnp.bfloat16),
                pltpu.VMEM((pool, width), jnp.bfloat16),
                pltpu.VMEM((rounds, 1, batch), jnp.int32),
                pltpu.VMEM((features, width), jnp.bfloat16),
                pltpu.SMEM(numerators.shape, jnp.int32),
                field, field, field, field, field, field,
                pltpu.VMEM((width, features), jnp.bfloat16),
                pltpu.VMEM((pool, features), jnp.bfloat16),
                arrivals, arrivals, arrivals, arrivals,
                pltpu.SemaphoreType.DMA((6,)),
                pltpu.SemaphoreType.DMA((2, 3 + PIECES)),
                pltpu.SemaphoreType.DMA((2, 3 + PIECES)),
            ],
            compiler_params=pltpu.CompilerParams(
                collective_id=0, has_side_effects=True, vmem_limit_bytes=54_000_000
            ),
        )(
            value_proj.reshape(width, features),
            token_pool.reshape(pool, width),
            target_pool.reshape(pool, width),
            batch_ids.reshape(rounds, 1, batch),
            frozen_out,
            numerators,
        )
        final_proj, final_tracker = pl.pallas_call(
            write_out,
            out_shape=(shape, shape),
            in_specs=[pl.BlockSpec(memory_space=pltpu.VMEM)] * 2,
            out_specs=(in_hbm,) * 2,
            scratch_shapes=[pltpu.SemaphoreType.DMA((2, OUT_PIECES))],
            compiler_params=pltpu.CompilerParams(vmem_limit_bytes=2**20),
        )(final_proj, final_tracker)
        return final_proj[None, None], final_tracker[None, None]

    return jax.shard_map(
        on_device,
        mesh=mesh,
        in_specs=(
            P("row", "col", None, None),
            P("row", "col", None, None),
            P("row", "col", None, None),
            P("row", "col", None, None),
            P(),
            P(),
        ),
        out_specs=(P("row", "col", None, None), P("row", "col", None, None)),
        check_vma=False,
    )
```

```python
import functools
import math

import jax
import jax.numpy as jnp
from jax import lax
from jax.experimental import pallas as pl
from jax.experimental.pallas import tpu as pltpu
from jax.sharding import PartitionSpec as P

MESH = pl.DeviceIdType.MESH
step_rate = 0.2
HEAD = 64
AXES = ("row", "col")


def kernel(sizes, x0_ref, tok_hbm, tgt_hbm, ids_hbm, fo_hbm, num_hbm, outx_ref, outy_ref,
           tok, tgt, ids, fo, num_ref, x0, x1, g0, g1, g2, y1, xb, bp,
           x0_in, g0_in, x1_in, y1_in, far_in, relay_in,
           local_sem, send_sem, recv_sem, extra_send, extra_recv, ready):
    pool, width = tok.shape
    features = x0.shape[1]
    factor = width ** (-0.5)
    f32, bf16 = jnp.float32, jnp.bfloat16
    right, left = {}, {}
    for axis, n in zip(AXES, sizes):
        me = lax.axis_index(axis)
        right[axis], left[axis] = lax.rem(me + 1, n), lax.rem(me + n - 1, n)
    n_col = sizes[1]
    col = lax.axis_index("col")
    first, last, before = col == 0, col == n_col - 1, col == n_col - 2
    size = min(HEAD, width // 2)
    head, rest = pl.ds(0, size), pl.ds(size, width - size)
    bulk, tail = pl.ds(0, width - size), pl.ds(width - size, size)

    load_head = pltpu.make_async_copy(x0_ref.at[head], x0.at[head], local_sem.at[0])
    load_head.start()

    barrier = pltpu.get_barrier_semaphore()

    def greet(axis, there):
        pl.semaphore_signal(barrier, inc=1, device_id={axis: there}, device_id_type=MESH)

    @pl.when(first)
    def _():
        greet("col", n_col - 2)

    @pl.when(jnp.logical_not(last))
    def _():
        greet("col", left["col"])

    @pl.when(before)
    def _():
        greet("col", n_col - 1)

    greet("row", left["row"])

    def copy_to(source, target, sends, recvs, device):
        return pltpu.make_async_remote_copy(
            src_ref=source, dst_ref=target, send_sem=sends, recv_sem=recvs,
            device_id=device, device_id_type=MESH,
        )

    def describe(source, target, which, slot):
        return copy_to(
            source, target, send_sem.at[which, slot], recv_sem.at[which, slot],
            {AXES[which]: right[AXES[which]]},
        )

    def describe_both(source, target, slot, rows):
        return [
            describe(source.at[rows], target.at[which, rows], which, slot) for which in (1, 0)
        ]

    far_copy = copy_to(
        x0.at[head], far_in, extra_send.at[0], extra_recv.at[0], {"col": 0}
    )
    relay_copy = copy_to(
        x0_in.at[1, head], relay_in, extra_send.at[1], extra_recv.at[1], {"row": right["row"]}
    )

    @pl.when(jnp.logical_not(last))
    def _():
        pl.semaphore_wait(barrier, 2)

    @pl.when(last)
    def _():
        pl.semaphore_wait(barrier, 3)
        pl.semaphore_signal(
            ready, inc=1, device_id={"col": n_col - 2}, device_id_type=MESH
        )

    load_head.wait()

    @pl.when(before)
    def _():
        far_copy.start()
        pl.semaphore_wait(ready, 1)

    x0_copies = describe_both(x0, x0_in, 0, head) + describe_both(x0_ref, x0_in, 1, rest)
    for copy in x0_copies:
        copy.start()

    loads = []
    for slot, (source, target) in enumerate(
        (
            (x0_ref.at[rest], x0.at[rest]), (tok_hbm, tok), (fo_hbm, fo),
            (tgt_hbm, tgt), (ids_hbm, ids), (num_hbm, num_ref),
        )
    ):
        load = pltpu.make_async_copy(source, target, local_sem.at[slot + 1])
        load.start()
        loads.append(load)

    step = math.gcd(width, 64)

    def by_rows(first, last, body):
        def go(i, carry):
            body(pl.ds(pl.multiple_of(i * step, step), step))
            return carry

        lax.fori_loop(first // step, last // step, go, 0)

    def mixed(own, arrived, rows):
        return w[0] * own[rows, :] + w[1] * arrived[0, rows, :] + w[2] * arrived[1, rows, :]

    block = math.gcd(pool, 256)
    wide = math.gcd(width, 256)

    def gradient(which, out):
        def forward(i, carry):
            rows = pl.ds(pl.multiple_of(i * block, block), block)
            preact = jnp.dot(tok[rows, :], xb[...], preferred_element_type=f32) * factor
            s = jax.nn.sigmoid(preact)
            hidden = (preact * s).astype(bf16)
            output = jnp.dot(hidden, fo[...], preferred_element_type=f32)
            error_term = (output - tgt[rows, :].astype(f32)).astype(bf16)
            back_hidden = lax.dot_general(
                error_term, fo[...], (((1,), (1,)), ((), ())), preferred_element_type=f32
            )
            slope = s * (1.0 + preact * (1.0 - s))
            row_ids = lax.broadcasted_iota(jnp.int32, (block, ids.shape[2]), 0) + i * block
            hits = jnp.where(row_ids == ids[which], 1.0, 0.0)
            times = jnp.sum(hits, axis=1, keepdims=True)
            bp[rows, :] = (back_hidden * slope * times).astype(bf16)
            return carry

        lax.fori_loop(0, pool // block, forward, 0)

        for j in range(width // wide):
            cols = pl.ds(j * wide, wide)
            out[cols, :] = (
                lax.dot_general(
                    tok[:, cols], bp[...], (((0,), (0,)), ((), ())), preferred_element_type=f32
                )
                * factor
            )

    for load in loads:
        load.wait()

    counts = [jnp.full((8, 128), num_ref[i], jnp.int32).astype(f32) for i in range(3)]
    total = counts[0] + counts[1] + counts[2]
    w = [(c / total)[0:1, 0:1] for c in counts]

    def first_round(rows):
        xb[rows, :] = x0[rows, :].astype(bf16)

    by_rows(0, width, first_round)
    gradient(0, g0)
    g0_copies = describe_both(g0, g0_in, 2, pl.ds(0, width))
    for copy in g0_copies:
        copy.start()

    for copy in x0_copies:
        copy.wait()

    @pl.when(first)
    def _():
        relay_copy.start()

    def first_move(rows):
        moved = mixed(x0, x0_in, rows) - step_rate * g0[rows, :]
        x1[rows, :] = moved
        xb[rows, :] = moved.astype(bf16)

    by_rows(0, width, first_move)
    x1_head, x1_head_row = describe_both(x1, x1_in, 3, head)
    x1_copies = [x1_head_row] + describe_both(x1, x1_in, 4, rest)

    @pl.when(jnp.logical_not(last))
    def _():
        x1_head.start()

    for copy in x1_copies:
        copy.start()
    gradient(1, g1)
    for copy in g0_copies:
        copy.wait()

    def first_track(rows):
        y1[rows, :] = mixed(g0, g0_in, rows) + g1[rows, :] - g0[rows, :]

    by_rows(0, width, first_track)
    y1_bulk = describe_both(y1, y1_in, 5, bulk)
    y1_tail = describe_both(y1, y1_in, 6, tail)
    for copy in y1_bulk + y1_tail:
        copy.start()

    for copy in x1_copies:
        copy.wait()

    @pl.when(jnp.logical_not(last))
    def _():
        x1_head.wait_send()

    @pl.when(jnp.logical_not(first))
    def _():
        x1_head.wait_recv()

    @pl.when(before)
    def _():
        far_copy.wait_send()

    @pl.when(first)
    def _():
        relay_copy.wait()
        far_copy.wait_recv()

        def neighbour_move(rows):
            x1_in[1, rows, :] = (
                w[0] * x0_in[1, rows, :]
                + w[1] * relay_in[rows, :]
                + w[2] * far_in[rows, :]
                - step_rate * g0_in[1, rows, :]
            )

        by_rows(0, size, neighbour_move)

    def second_move(rows):
        moved = mixed(x1, x1_in, rows) - step_rate * y1[rows, :]
        outx_ref[rows, :] = moved
        xb[rows, :] = moved.astype(bf16)

    by_rows(0, width, second_move)
    gradient(2, g2)

    def second_track(rows):
        outy_ref[rows, :] = mixed(y1, y1_in, rows) + g2[rows, :] - g1[rows, :]

    for copy in y1_bulk:
        copy.wait()
    by_rows(0, width - size, second_track)
    for copy in y1_tail:
        copy.wait()
    by_rows(width - size, width, second_track)


def write_out(x_ref, y_ref, x_hbm, y_hbm, sems):
    copies = []
    for slot, (source, target) in enumerate(((x_ref, x_hbm), (y_ref, y_hbm))):
        copy = pltpu.make_async_copy(source, target, sems.at[slot])
        copy.start()
        copies.append(copy)
    for copy in copies:
        copy.wait()


def solution(mesh):
    sizes = tuple(mesh.shape[axis] for axis in AXES)

    def on_device(value_proj, token_pool, target_pool, batch_ids, frozen_out, numerators):
        width, features = value_proj.shape[2:]
        pool = token_pool.shape[2]
        rounds, batch = batch_ids.shape[2:]
        field = pltpu.VMEM((width, features), jnp.float32)
        arrivals = pltpu.VMEM((2, width, features), jnp.float32)
        in_hbm = pl.BlockSpec(memory_space=pltpu.HBM)
        shape = jax.ShapeDtypeStruct((width, features), jnp.float32)
        final_proj, final_tracker = pl.pallas_call(
            functools.partial(kernel, sizes),
            out_shape=(pltpu.VMEM((width, features), jnp.float32),) * 2,
            in_specs=[in_hbm] * 6,
            out_specs=(pl.BlockSpec(memory_space=pltpu.VMEM),) * 2,
            scratch_shapes=[
                pltpu.VMEM((pool, width), jnp.bfloat16),
                pltpu.VMEM((pool, width), jnp.bfloat16),
                pltpu.VMEM((rounds, 1, batch), jnp.int32),
                pltpu.VMEM((features, width), jnp.bfloat16),
                pltpu.SMEM(numerators.shape, jnp.int32),
                field, field, field, field, field, field,
                pltpu.VMEM((width, features), jnp.bfloat16),
                pltpu.VMEM((pool, features), jnp.bfloat16),
                arrivals, arrivals, arrivals, arrivals,
                pltpu.VMEM((min(HEAD, width // 2), features), jnp.float32),
                pltpu.VMEM((min(HEAD, width // 2), features), jnp.float32),
                pltpu.SemaphoreType.DMA((7,)),
                pltpu.SemaphoreType.DMA((2, 7)),
                pltpu.SemaphoreType.DMA((2, 7)),
                pltpu.SemaphoreType.DMA((2,)),
                pltpu.SemaphoreType.DMA((2,)),
                pltpu.SemaphoreType.REGULAR,
            ],
            compiler_params=pltpu.CompilerParams(
                collective_id=0, has_side_effects=True, vmem_limit_bytes=54_000_000
            ),
        )(
            value_proj.reshape(width, features),
            token_pool.reshape(pool, width),
            target_pool.reshape(pool, width),
            batch_ids.reshape(rounds, 1, batch),
            frozen_out,
            numerators,
        )
        final_proj, final_tracker = pl.pallas_call(
            write_out,
            out_shape=(shape, shape),
            in_specs=[pl.BlockSpec(memory_space=pltpu.VMEM)] * 2,
            out_specs=(in_hbm,) * 2,
            scratch_shapes=[pltpu.SemaphoreType.DMA((2,))],
            compiler_params=pltpu.CompilerParams(vmem_limit_bytes=2**20),
        )(final_proj, final_tracker)
        return final_proj[None, None], final_tracker[None, None]

    return jax.shard_map(
        on_device,
        mesh=mesh,
        in_specs=(
            P("row", "col", None, None),
            P("row", "col", None, None),
            P("row", "col", None, None),
            P("row", "col", None, None),
            P(),
            P(),
        ),
        out_specs=(P("row", "col", None, None), P("row", "col", None, None)),
        check_vma=False,
    )
```

```python
import functools
import math

import jax
import jax.numpy as jnp
from jax import lax
from jax.experimental import pallas as pl
from jax.experimental.pallas import tpu as pltpu
from jax.sharding import PartitionSpec as P

MESH = pl.DeviceIdType.MESH
step_rate = 0.2
PIECES = 8
EARLY = 3
AXES = ("row", "col")


def kernel(sizes, x0_ref, tok_hbm, tgt_hbm, ids_hbm, fo_hbm, num_hbm, outx_ref, outy_ref,
           tok, tgt, ids, fo, num_ref, x0, x1, g0, g1, g2, y1, xb, bp,
           x0_in, g0_in, x1_in, y1_in, far_in, mix2, mix3,
           local_sem, send_sem, recv_sem, far_send, far_recv):
    pool, width = tok.shape
    features = x0.shape[1]
    factor = width ** (-0.5)
    f32, bf16 = jnp.float32, jnp.bfloat16
    piece = width // PIECES
    right, left = {}, {}
    for axis, n in zip(AXES, sizes):
        me = lax.axis_index(axis)
        right[axis], left[axis] = lax.rem(me + 1, n), lax.rem(me + n - 1, n)

    n_col = sizes[1]
    col = lax.axis_index("col")
    first, second, last = col == 0, col == 1, col == n_col - 1

    def where(condition):
        return pl.when(condition), pl.when(jnp.logical_not(condition))

    barrier = pltpu.get_barrier_semaphore()
    for axis in AXES:
        pl.semaphore_signal(
            barrier, inc=1, device_id={axis: left[axis]}, device_id_type=MESH
        )

    @pl.when(second)
    def _():
        pl.semaphore_signal(
            barrier, inc=1, device_id={"col": n_col - 1}, device_id_type=MESH
        )

    on_last, elsewhere = where(last)

    @on_last
    def _():
        pl.semaphore_wait(barrier, 3)

    @elsewhere
    def _():
        pl.semaphore_wait(barrier, 2)

    def describe(source, target, which, slot):
        return pltpu.make_async_remote_copy(
            src_ref=source,
            dst_ref=target,
            send_sem=send_sem.at[which, slot],
            recv_sem=recv_sem.at[which, slot],
            device_id={AXES[which]: right[AXES[which]]},
            device_id_type=MESH,
        )

    def send_rows(source, target, slot, rows, other=None):
        by_col = describe(source.at[rows], target.at[1, rows], 1, slot)
        by_row = describe(source.at[rows], target.at[0, rows], 0, slot)
        if other is None:
            by_col.start()
        else:
            @elsewhere
            def _():
                by_col.start()

            @on_last
            def _():
                describe(other.at[rows], target.at[1, rows], 1, slot).start()

        by_row.start()
        return [by_col, by_row]

    whole = pl.ds(0, width)
    x0_copies = send_rows(x0_ref, x0_in, 0, whole)

    loads = []
    for slot, (source, target) in enumerate(
        (
            (x0_ref, x0), (tok_hbm, tok), (fo_hbm, fo),
            (tgt_hbm, tgt), (ids_hbm, ids), (num_hbm, num_ref),
        )
    ):
        load = pltpu.make_async_copy(source, target, local_sem.at[slot])
        load.start()
        loads.append(load)

    step = math.gcd(width, 64)

    def by_rows(first, last, body):
        def go(i, carry):
            body(pl.ds(pl.multiple_of(i * step, step), step))
            return carry

        lax.fori_loop(first // step, last // step, go, 0)

    def mixed(own, arrived, rows):
        return w[0] * own[rows, :] + w[1] * arrived[0, rows, :] + w[2] * arrived[1, rows, :]

    block = math.gcd(pool, 256)
    wide = math.gcd(width, 256)

    def gradient(which, out):
        def forward(i, carry):
            rows = pl.ds(pl.multiple_of(i * block, block), block)
            preact = jnp.dot(tok[rows, :], xb[...], preferred_element_type=f32) * factor
            s = jax.nn.sigmoid(preact)
            hidden = (preact * s).astype(bf16)
            output = jnp.dot(hidden, fo[...], preferred_element_type=f32)
            error_term = (output - tgt[rows, :].astype(f32)).astype(bf16)
            back_hidden = lax.dot_general(
                error_term, fo[...], (((1,), (1,)), ((), ())), preferred_element_type=f32
            )
            slope = s * (1.0 + preact * (1.0 - s))
            row_ids = lax.broadcasted_iota(jnp.int32, (block, ids.shape[2]), 0) + i * block
            hits = jnp.where(row_ids == ids[which], 1.0, 0.0)
            times = jnp.sum(hits, axis=1, keepdims=True)
            bp[rows, :] = (back_hidden * slope * times).astype(bf16)
            return carry

        lax.fori_loop(0, pool // block, forward, 0)

        for j in range(width // wide):
            cols = pl.ds(j * wide, wide)
            out[cols, :] = (
                lax.dot_general(
                    tok[:, cols], bp[...], (((0,), (0,)), ((), ())), preferred_element_type=f32
                )
                * factor
            )

    for load in loads:
        load.wait()

    counts = [jnp.full((8, 128), num_ref[i], jnp.int32).astype(f32) for i in range(3)]
    total = counts[0] + counts[1] + counts[2]
    w = [(c / total)[0:1, 0:1] for c in counts]

    def first_round(rows):
        xb[rows, :] = x0[rows, :].astype(bf16)

    by_rows(0, width, first_round)
    gradient(0, g0)
    g0_col = describe(g0, g0_in.at[1], 1, 1)
    g0_row = describe(g0, g0_in.at[0], 0, 1)
    g0_row.start()

    far_copies = []
    for part in range(PIECES):
        rows = pl.ds(part * piece, piece)
        far_copies.append(
            pltpu.make_async_remote_copy(
                src_ref=g0.at[rows], dst_ref=far_in.at[rows],
                send_sem=far_send.at[part], recv_sem=far_recv.at[part],
                device_id={"col": 1}, device_id_type=MESH,
            )
        )

    @elsewhere
    def _():
        g0_col.start()

    @on_last
    def _():
        for copy in far_copies[:EARLY]:
            copy.start()

    for copy in x0_copies:
        copy.wait()

    def first_move(rows):
        moved = mixed(x0, x0_in, rows) - step_rate * g0[rows, :]
        x1[rows, :] = moved
        xb[rows, :] = moved.astype(bf16)

    by_rows(0, width, first_move)

    @on_last
    def _():
        def make_mix2(rows):
            mix2[rows, :] = x1[rows, :] - step_rate * g0[rows, :]

        by_rows(0, width, make_mix2)

    x1_copies = send_rows(x1, x1_in, 2, whole, mix2)
    gradient(1, g1)
    g0_row.wait()
    on_first, beyond = where(first)

    @on_first
    def _():
        def first_track(rows):
            y1[rows, :] = (
                w[0] * g0[rows, :] + w[1] * g0_in[0, rows, :] + g1[rows, :] - g0[rows, :]
            )

        by_rows(0, width, first_track)

    @beyond
    def _():
        g0_col.wait_recv()

        def first_track(rows):
            y1[rows, :] = mixed(g0, g0_in, rows) + g1[rows, :] - g0[rows, :]

        by_rows(0, width, first_track)

    @on_last
    def _():
        def make_mix3(rows):
            mix3[rows, :] = y1[rows, :] + w[0] * g0[rows, :] + w[1] * g0_in[0, rows, :]

        by_rows(0, width, make_mix3)

    y1_copies = [
        send_rows(y1, y1_in, 3 + part, pl.ds(part * piece, piece), mix3)
        for part in range(PIECES)
    ]

    @elsewhere
    def _():
        g0_col.wait_send()

    @on_last
    def _():
        for copy in far_copies[EARLY:]:
            copy.start()

    for copy in x1_copies:
        copy.wait()

    def second_move(rows):
        moved = mixed(x1, x1_in, rows) - step_rate * y1[rows, :]
        outx_ref[rows, :] = moved
        xb[rows, :] = moved.astype(bf16)

    by_rows(0, width, second_move)
    gradient(2, g2)

    def second_track(rows):
        outy_ref[rows, :] = mixed(y1, y1_in, rows) + g2[rows, :] - g1[rows, :]

    def second_track_far(rows):
        second = w[2] * (y1_in[1, rows, :] + w[2] * far_in[rows, :])
        outy_ref[rows, :] = (
            w[0] * y1[rows, :] + w[1] * y1_in[0, rows, :] + second
            + g2[rows, :] - g1[rows, :]
        )

    on_second, others = where(second)
    for part in range(PIECES):
        for copy in y1_copies[part]:
            copy.wait()

        @on_second
        def _(part=part):
            far_copies[part].wait_recv()
            by_rows(part * piece, (part + 1) * piece, second_track_far)

        @others
        def _(part=part):
            by_rows(part * piece, (part + 1) * piece, second_track)

    @on_last
    def _():
        for copy in far_copies:
            copy.wait_send()


def write_out(x_ref, y_ref, x_hbm, y_hbm, sems):
    copies = []
    for slot, (source, target) in enumerate(((x_ref, x_hbm), (y_ref, y_hbm))):
        copy = pltpu.make_async_copy(source, target, sems.at[slot])
        copy.start()
        copies.append(copy)
    for copy in copies:
        copy.wait()


def solution(mesh):
    sizes = tuple(mesh.shape[axis] for axis in AXES)

    def on_device(value_proj, token_pool, target_pool, batch_ids, frozen_out, numerators):
        width, features = value_proj.shape[2:]
        pool = token_pool.shape[2]
        rounds, batch = batch_ids.shape[2:]
        field = pltpu.VMEM((width, features), jnp.float32)
        arrivals = pltpu.VMEM((2, width, features), jnp.float32)
        in_hbm = pl.BlockSpec(memory_space=pltpu.HBM)
        shape = jax.ShapeDtypeStruct((width, features), jnp.float32)
        final_proj, final_tracker = pl.pallas_call(
            functools.partial(kernel, sizes),
            out_shape=(pltpu.VMEM((width, features), jnp.float32),) * 2,
            in_specs=[in_hbm] * 6,
            out_specs=(pl.BlockSpec(memory_space=pltpu.VMEM),) * 2,
            scratch_shapes=[
                pltpu.VMEM((pool, width), jnp.bfloat16),
                pltpu.VMEM((pool, width), jnp.bfloat16),
                pltpu.VMEM((rounds, 1, batch), jnp.int32),
                pltpu.VMEM((features, width), jnp.bfloat16),
                pltpu.SMEM(numerators.shape, jnp.int32),
                field, field, field, field, field, field,
                pltpu.VMEM((width, features), jnp.bfloat16),
                pltpu.VMEM((pool, features), jnp.bfloat16),
                arrivals, arrivals, arrivals, arrivals,
                field, field, field,
                pltpu.SemaphoreType.DMA((6,)),
                pltpu.SemaphoreType.DMA((2, 3 + PIECES)),
                pltpu.SemaphoreType.DMA((2, 3 + PIECES)),
                pltpu.SemaphoreType.DMA((PIECES,)),
                pltpu.SemaphoreType.DMA((PIECES,)),
            ],
            compiler_params=pltpu.CompilerParams(
                collective_id=0, has_side_effects=True, vmem_limit_bytes=54_000_000
            ),
        )(
            value_proj.reshape(width, features),
            token_pool.reshape(pool, width),
            target_pool.reshape(pool, width),
            batch_ids.reshape(rounds, 1, batch),
            frozen_out,
            numerators,
        )
        final_proj, final_tracker = pl.pallas_call(
            write_out,
            out_shape=(shape, shape),
            in_specs=[pl.BlockSpec(memory_space=pltpu.VMEM)] * 2,
            out_specs=(in_hbm,) * 2,
            scratch_shapes=[pltpu.SemaphoreType.DMA((2,))],
            compiler_params=pltpu.CompilerParams(vmem_limit_bytes=2**20),
        )(final_proj, final_tracker)
        return final_proj[None, None], final_tracker[None, None]

    return jax.shard_map(
        on_device,
        mesh=mesh,
        in_specs=(
            P("row", "col", None, None),
            P("row", "col", None, None),
            P("row", "col", None, None),
            P("row", "col", None, None),
            P(),
            P(),
        ),
        out_specs=(P("row", "col", None, None), P("row", "col", None, None)),
        check_vma=False,
    )
```

```python
import functools
import math

import jax
import jax.numpy as jnp
from jax import lax
from jax.experimental import pallas as pl
from jax.experimental.pallas import tpu as pltpu
from jax.sharding import PartitionSpec as P

MESH = pl.DeviceIdType.MESH
step_rate = 0.2
PIECES = 8
EARLY = 3
AXES = ("row", "col")


def kernel(sizes, x0_ref, tok_hbm, tgt_hbm, ids_hbm, fo_hbm, num_hbm, outx_ref, outy_ref,
           tok, tgt, ids, fo, num_ref, x0, x1, g0, g1, g2, y1, xb, bp,
           x0_in, g0_in, x1_in, y1_in, far_in, mix2, mix3,
           local_sem, send_sem, recv_sem, far_send, far_recv, row_ready):
    pool, width = tok.shape
    features = x0.shape[1]
    factor = width ** (-0.5)
    f32, bf16 = jnp.float32, jnp.bfloat16
    piece = width // PIECES
    right, left = {}, {}
    for axis, n in zip(AXES, sizes):
        me = lax.axis_index(axis)
        right[axis], left[axis] = lax.rem(me + 1, n), lax.rem(me + n - 1, n)

    n_col = sizes[1]
    col = lax.axis_index("col")
    first, second, last = col == 0, col == 1, col == n_col - 1

    def where(condition):
        return pl.when(condition), pl.when(jnp.logical_not(condition))

    barrier = pltpu.get_barrier_semaphore()
    for there in ({"col": left["col"]}, {"row": right["row"]}):
        pl.semaphore_signal(barrier, inc=1, device_id=there, device_id_type=MESH)

    @pl.when(second)
    def _():
        pl.semaphore_signal(
            barrier, inc=1, device_id={"col": n_col - 1}, device_id_type=MESH
        )

    on_last, elsewhere = where(last)

    @on_last
    def _():
        pl.semaphore_wait(barrier, 3)

    @elsewhere
    def _():
        pl.semaphore_wait(barrier, 2)

    def describe(source, target, which, slot):
        return pltpu.make_async_remote_copy(
            src_ref=source,
            dst_ref=target,
            send_sem=send_sem.at[which, slot],
            recv_sem=recv_sem.at[which, slot],
            device_id={AXES[which]: right[AXES[which]]},
            device_id_type=MESH,
        )

    def send_rows(source, target, slot, rows, other=None):
        by_col = describe(source.at[rows], target.at[1, rows], 1, slot)
        by_row = describe(source.at[rows], target.at[0, rows], 0, slot)
        if other is None:
            by_col.start()
        else:
            @elsewhere
            def _():
                by_col.start()

            @on_last
            def _():
                describe(other.at[rows], target.at[1, rows], 1, slot).start()

        by_row.start()
        return [by_col, by_row]

    whole = pl.ds(0, width)
    x0_copies = [describe(x0_ref, x0_in.at[which], which, 0) for which in (1, 0)]
    x0_copies[0].start()
    pl.semaphore_signal(row_ready, inc=1, device_id={"row": left["row"]}, device_id_type=MESH)
    pl.semaphore_wait(row_ready, 1)
    x0_copies[1].start()

    loads = []
    for slot, (source, target) in enumerate(
        (
            (x0_ref, x0), (tok_hbm, tok), (fo_hbm, fo),
            (tgt_hbm, tgt), (ids_hbm, ids), (num_hbm, num_ref),
        )
    ):
        load = pltpu.make_async_copy(source, target, local_sem.at[slot])
        load.start()
        loads.append(load)

    step = math.gcd(width, 64)

    def by_rows(first, last, body):
        def go(i, carry):
            body(pl.ds(pl.multiple_of(i * step, step), step))
            return carry

        lax.fori_loop(first // step, last // step, go, 0)

    def mixed(own, arrived, rows):
        return w[0] * own[rows, :] + w[1] * arrived[0, rows, :] + w[2] * arrived[1, rows, :]

    block = math.gcd(pool, 256)
    wide = math.gcd(width, 256)

    def gradient(which, out):
        def forward(i, carry):
            rows = pl.ds(pl.multiple_of(i * block, block), block)
            preact = jnp.dot(tok[rows, :], xb[...], preferred_element_type=f32) * factor
            s = jax.nn.sigmoid(preact)
            hidden = (preact * s).astype(bf16)
            output = jnp.dot(hidden, fo[...], preferred_element_type=f32)
            error_term = (output - tgt[rows, :].astype(f32)).astype(bf16)
            back_hidden = lax.dot_general(
                error_term, fo[...], (((1,), (1,)), ((), ())), preferred_element_type=f32
            )
            slope = s * (1.0 + preact * (1.0 - s))
            row_ids = lax.broadcasted_iota(jnp.int32, (block, ids.shape[2]), 0) + i * block
            hits = jnp.where(row_ids == ids[which], 1.0, 0.0)
            times = jnp.sum(hits, axis=1, keepdims=True)
            bp[rows, :] = (back_hidden * slope * times).astype(bf16)
            return carry

        lax.fori_loop(0, pool // block, forward, 0)

        for j in range(width // wide):
            cols = pl.ds(j * wide, wide)
            out[cols, :] = (
                lax.dot_general(
                    tok[:, cols], bp[...], (((0,), (0,)), ((), ())), preferred_element_type=f32
                )
                * factor
            )

    for load in loads:
        load.wait()

    counts = [jnp.full((8, 128), num_ref[i], jnp.int32).astype(f32) for i in range(3)]
    total = counts[0] + counts[1] + counts[2]
    w = [(c / total)[0:1, 0:1] for c in counts]

    def first_round(rows):
        xb[rows, :] = x0[rows, :].astype(bf16)

    by_rows(0, width, first_round)
    gradient(0, g0)
    g0_col = describe(g0, g0_in.at[1], 1, 1)
    g0_row = describe(g0, g0_in.at[0], 0, 1)
    g0_row.start()

    far_copies = []
    for part in range(PIECES):
        rows = pl.ds(part * piece, piece)
        far_copies.append(
            pltpu.make_async_remote_copy(
                src_ref=g0.at[rows], dst_ref=far_in.at[rows],
                send_sem=far_send.at[part], recv_sem=far_recv.at[part],
                device_id={"col": 1}, device_id_type=MESH,
            )
        )

    @elsewhere
    def _():
        g0_col.start()

    @on_last
    def _():
        for copy in far_copies[:EARLY]:
            copy.start()

    for copy in x0_copies:
        copy.wait()

    def first_move(rows):
        moved = mixed(x0, x0_in, rows) - step_rate * g0[rows, :]
        x1[rows, :] = moved
        xb[rows, :] = moved.astype(bf16)

    by_rows(0, width, first_move)

    @on_last
    def _():
        def make_mix2(rows):
            mix2[rows, :] = x1[rows, :] - step_rate * g0[rows, :]

        by_rows(0, width, make_mix2)

    x1_copies = send_rows(x1, x1_in, 2, whole, mix2)
    gradient(1, g1)
    g0_row.wait()
    on_first, beyond = where(first)

    @on_first
    def _():
        def first_track(rows):
            y1[rows, :] = (
                w[0] * g0[rows, :] + w[1] * g0_in[0, rows, :] + g1[rows, :] - g0[rows, :]
            )

        by_rows(0, width, first_track)

    @beyond
    def _():
        g0_col.wait_recv()

        def first_track(rows):
            y1[rows, :] = mixed(g0, g0_in, rows) + g1[rows, :] - g0[rows, :]

        by_rows(0, width, first_track)

    @on_last
    def _():
        def make_mix3(rows):
            mix3[rows, :] = y1[rows, :] + w[0] * g0[rows, :] + w[1] * g0_in[0, rows, :]

        by_rows(0, width, make_mix3)

    y1_copies = [
        send_rows(y1, y1_in, 3 + part, pl.ds(part * piece, piece), mix3)
        for part in range(PIECES)
    ]

    @elsewhere
    def _():
        g0_col.wait_send()

    @on_last
    def _():
        for copy in far_copies[EARLY:]:
            copy.start()

    for copy in x1_copies:
        copy.wait()

    def second_move(rows):
        moved = mixed(x1, x1_in, rows) - step_rate * y1[rows, :]
        outx_ref[rows, :] = moved
        xb[rows, :] = moved.astype(bf16)

    by_rows(0, width, second_move)
    gradient(2, g2)

    def second_track(rows):
        outy_ref[rows, :] = mixed(y1, y1_in, rows) + g2[rows, :] - g1[rows, :]

    def second_track_far(rows):
        second = w[2] * (y1_in[1, rows, :] + w[2] * far_in[rows, :])
        outy_ref[rows, :] = (
            w[0] * y1[rows, :] + w[1] * y1_in[0, rows, :] + second
            + g2[rows, :] - g1[rows, :]
        )

    on_second, others = where(second)
    for part in range(PIECES):
        for copy in y1_copies[part]:
            copy.wait()

        @on_second
        def _(part=part):
            far_copies[part].wait_recv()
            by_rows(part * piece, (part + 1) * piece, second_track_far)

        @others
        def _(part=part):
            by_rows(part * piece, (part + 1) * piece, second_track)

    @on_last
    def _():
        for copy in far_copies:
            copy.wait_send()


def write_out(x_ref, y_ref, x_hbm, y_hbm, sems):
    copies = []
    for slot, (source, target) in enumerate(((x_ref, x_hbm), (y_ref, y_hbm))):
        copy = pltpu.make_async_copy(source, target, sems.at[slot])
        copy.start()
        copies.append(copy)
    for copy in copies:
        copy.wait()


def solution(mesh):
    sizes = tuple(mesh.shape[axis] for axis in AXES)

    def on_device(value_proj, token_pool, target_pool, batch_ids, frozen_out, numerators):
        width, features = value_proj.shape[2:]
        pool = token_pool.shape[2]
        rounds, batch = batch_ids.shape[2:]
        field = pltpu.VMEM((width, features), jnp.float32)
        arrivals = pltpu.VMEM((2, width, features), jnp.float32)
        in_hbm = pl.BlockSpec(memory_space=pltpu.HBM)
        shape = jax.ShapeDtypeStruct((width, features), jnp.float32)
        final_proj, final_tracker = pl.pallas_call(
            functools.partial(kernel, sizes),
            out_shape=(pltpu.VMEM((width, features), jnp.float32),) * 2,
            in_specs=[in_hbm] * 6,
            out_specs=(pl.BlockSpec(memory_space=pltpu.VMEM),) * 2,
            scratch_shapes=[
                pltpu.VMEM((pool, width), jnp.bfloat16),
                pltpu.VMEM((pool, width), jnp.bfloat16),
                pltpu.VMEM((rounds, 1, batch), jnp.int32),
                pltpu.VMEM((features, width), jnp.bfloat16),
                pltpu.SMEM(numerators.shape, jnp.int32),
                field, field, field, field, field, field,
                pltpu.VMEM((width, features), jnp.bfloat16),
                pltpu.VMEM((pool, features), jnp.bfloat16),
                arrivals, arrivals, arrivals, arrivals,
                field, field, field,
                pltpu.SemaphoreType.DMA((6,)),
                pltpu.SemaphoreType.DMA((2, 3 + PIECES)),
                pltpu.SemaphoreType.DMA((2, 3 + PIECES)),
                pltpu.SemaphoreType.DMA((PIECES,)),
                pltpu.SemaphoreType.DMA((PIECES,)),
                pltpu.SemaphoreType.REGULAR,
            ],
            compiler_params=pltpu.CompilerParams(
                collective_id=0, has_side_effects=True, vmem_limit_bytes=54_000_000
            ),
        )(
            value_proj.reshape(width, features),
            token_pool.reshape(pool, width),
            target_pool.reshape(pool, width),
            batch_ids.reshape(rounds, 1, batch),
            frozen_out,
            numerators,
        )
        final_proj, final_tracker = pl.pallas_call(
            write_out,
            out_shape=(shape, shape),
            in_specs=[pl.BlockSpec(memory_space=pltpu.VMEM)] * 2,
            out_specs=(in_hbm,) * 2,
            scratch_shapes=[pltpu.SemaphoreType.DMA((2,))],
            compiler_params=pltpu.CompilerParams(vmem_limit_bytes=2**20),
        )(final_proj, final_tracker)
        return final_proj[None, None], final_tracker[None, None]

    return jax.shard_map(
        on_device,
        mesh=mesh,
        in_specs=(
            P("row", "col", None, None),
            P("row", "col", None, None),
            P("row", "col", None, None),
            P("row", "col", None, None),
            P(),
            P(),
        ),
        out_specs=(P("row", "col", None, None), P("row", "col", None, None)),
        check_vma=False,
    )
```

```python
import functools
import math

import jax
import jax.numpy as jnp
from jax import lax
from jax.experimental import pallas as pl
from jax.experimental.pallas import tpu as pltpu
from jax.sharding import PartitionSpec as P

MESH = pl.DeviceIdType.MESH
step_rate = 0.2
TAIL = 64
AXES = ("row", "col")


def kernel(sizes, x0_ref, tok_hbm, tgt_hbm, ids_hbm, fo_hbm, num_hbm, outx_ref, outy_ref,
           tok, tgt, ids, fo, num_ref, x0, x1, g0, g1, g2, y1, xb, bp,
           x0_in, g0_in, x1_in, y1_in, far_in, mix2, mix3,
           local_sem, send_sem, recv_sem, far_send, far_recv, row_ready):
    pool, width = tok.shape
    features = x0.shape[1]
    factor = width ** (-0.5)
    f32, bf16 = jnp.float32, jnp.bfloat16
    early, bulk = 3 * width // 8, width - min(TAIL, width // 8)
    right, left = {}, {}
    for axis, n in zip(AXES, sizes):
        me = lax.axis_index(axis)
        right[axis], left[axis] = lax.rem(me + 1, n), lax.rem(me + n - 1, n)

    n_col = sizes[1]
    col = lax.axis_index("col")
    first, second, last = col == 0, col == 1, col == n_col - 1

    def where(condition):
        return pl.when(condition), pl.when(jnp.logical_not(condition))

    barrier = pltpu.get_barrier_semaphore()
    for there in ({"col": left["col"]}, {"row": right["row"]}):
        pl.semaphore_signal(barrier, inc=1, device_id=there, device_id_type=MESH)

    @pl.when(second)
    def _():
        pl.semaphore_signal(
            barrier, inc=1, device_id={"col": n_col - 1}, device_id_type=MESH
        )

    on_last, elsewhere = where(last)

    @on_last
    def _():
        pl.semaphore_wait(barrier, 3)

    @elsewhere
    def _():
        pl.semaphore_wait(barrier, 2)

    def describe(source, target, which, slot):
        return pltpu.make_async_remote_copy(
            src_ref=source,
            dst_ref=target,
            send_sem=send_sem.at[which, slot],
            recv_sem=recv_sem.at[which, slot],
            device_id={AXES[which]: right[AXES[which]]},
            device_id_type=MESH,
        )

    def send_rows(source, target, slot, rows, other=None):
        by_col = describe(source.at[rows], target.at[1, rows], 1, slot)
        by_row = describe(source.at[rows], target.at[0, rows], 0, slot)
        if other is None:
            by_col.start()
        else:
            @elsewhere
            def _():
                by_col.start()

            @on_last
            def _():
                describe(other.at[rows], target.at[1, rows], 1, slot).start()

        by_row.start()
        return [by_col, by_row]

    whole = pl.ds(0, width)
    x0_copies = [describe(x0_ref, x0_in.at[which], which, 0) for which in (1, 0)]
    x0_copies[0].start()
    pl.semaphore_signal(row_ready, inc=1, device_id={"row": left["row"]}, device_id_type=MESH)
    pl.semaphore_wait(row_ready, 1)
    x0_copies[1].start()

    loads = []
    for slot, (source, target) in enumerate(
        (
            (x0_ref, x0), (tok_hbm, tok), (fo_hbm, fo),
            (tgt_hbm, tgt), (ids_hbm, ids), (num_hbm, num_ref),
        )
    ):
        load = pltpu.make_async_copy(source, target, local_sem.at[slot])
        load.start()
        loads.append(load)

    step = math.gcd(width, 64)

    def by_rows(first, last, body):
        def go(i, carry):
            body(pl.ds(pl.multiple_of(i * step, step), step))
            return carry

        lax.fori_loop(first // step, last // step, go, 0)

    def mixed(own, arrived, rows):
        return w[0] * own[rows, :] + w[1] * arrived[0, rows, :] + w[2] * arrived[1, rows, :]

    block = math.gcd(pool, 256)
    wide = math.gcd(width, 256)

    def gradient(which, out):
        def forward(i, carry):
            rows = pl.ds(pl.multiple_of(i * block, block), block)
            preact = jnp.dot(tok[rows, :], xb[...], preferred_element_type=f32) * factor
            s = jax.nn.sigmoid(preact)
            hidden = (preact * s).astype(bf16)
            output = jnp.dot(hidden, fo[...], preferred_element_type=f32)
            error_term = (output - tgt[rows, :].astype(f32)).astype(bf16)
            back_hidden = lax.dot_general(
                error_term, fo[...], (((1,), (1,)), ((), ())), preferred_element_type=f32
            )
            slope = s * (1.0 + preact * (1.0 - s))
            row_ids = lax.broadcasted_iota(jnp.int32, (block, ids.shape[2]), 0) + i * block
            hits = jnp.where(row_ids == ids[which], 1.0, 0.0)
            times = jnp.sum(hits, axis=1, keepdims=True)
            bp[rows, :] = (back_hidden * slope * times).astype(bf16)
            return carry

        lax.fori_loop(0, pool // block, forward, 0)

        for j in range(width // wide):
            cols = pl.ds(j * wide, wide)
            out[cols, :] = (
                lax.dot_general(
                    tok[:, cols], bp[...], (((0,), (0,)), ((), ())), preferred_element_type=f32
                )
                * factor
            )

    for load in loads:
        load.wait()

    counts = [jnp.full((8, 128), num_ref[i], jnp.int32).astype(f32) for i in range(3)]
    total = counts[0] + counts[1] + counts[2]
    w = [(c / total)[0:1, 0:1] for c in counts]

    def first_round(rows):
        xb[rows, :] = x0[rows, :].astype(bf16)

    by_rows(0, width, first_round)
    gradient(0, g0)
    g0_col = describe(g0, g0_in.at[1], 1, 1)
    g0_row = describe(g0, g0_in.at[0], 0, 1)
    g0_row.start()

    far_copies = []
    for part, (start, stop) in enumerate(((0, early), (early, bulk), (bulk, width))):
        rows = pl.ds(start, stop - start)
        far_copies.append(
            pltpu.make_async_remote_copy(
                src_ref=g0.at[rows], dst_ref=far_in.at[rows],
                send_sem=far_send.at[part], recv_sem=far_recv.at[part],
                device_id={"col": 1}, device_id_type=MESH,
            )
        )

    @elsewhere
    def _():
        g0_col.start()

    @on_last
    def _():
        far_copies[0].start()

    for copy in x0_copies:
        copy.wait()

    def first_move(rows):
        moved = mixed(x0, x0_in, rows) - step_rate * g0[rows, :]
        x1[rows, :] = moved
        xb[rows, :] = moved.astype(bf16)

    by_rows(0, width, first_move)

    @on_last
    def _():
        def make_mix2(rows):
            mix2[rows, :] = x1[rows, :] - step_rate * g0[rows, :]

        by_rows(0, width, make_mix2)

    x1_copies = send_rows(x1, x1_in, 2, whole, mix2)
    gradient(1, g1)
    g0_row.wait()
    on_first, beyond = where(first)

    @on_first
    def _():
        def first_track(rows):
            y1[rows, :] = (
                w[0] * g0[rows, :] + w[1] * g0_in[0, rows, :] + g1[rows, :] - g0[rows, :]
            )

        by_rows(0, width, first_track)

    @beyond
    def _():
        g0_col.wait_recv()

        def first_track(rows):
            y1[rows, :] = mixed(g0, g0_in, rows) + g1[rows, :] - g0[rows, :]

        by_rows(0, width, first_track)

    @on_last
    def _():
        def make_mix3(rows):
            mix3[rows, :] = y1[rows, :] + w[0] * g0[rows, :] + w[1] * g0_in[0, rows, :]

        by_rows(0, width, make_mix3)

    parts = ((0, bulk), (bulk, width))
    y1_copies = []
    for part, (start, stop) in enumerate(parts):
        rows = pl.ds(start, stop - start)
        by_col = describe(y1.at[rows], y1_in.at[1, rows], 1, 3 + part)

        @elsewhere
        def _(by_col=by_col):
            by_col.start()

        @on_last
        def _(rows=rows, part=part):
            describe(mix3.at[rows], y1_in.at[1, rows], 1, 3 + part).start()

        y1_copies.append([by_col])
    y1_row = describe(y1, y1_in.at[0], 0, 3)
    y1_row.start()

    @elsewhere
    def _():
        g0_col.wait_send()

    @on_last
    def _():
        for copy in far_copies[1:]:
            copy.start()

    for copy in x1_copies:
        copy.wait()

    def second_move(rows):
        moved = mixed(x1, x1_in, rows) - step_rate * y1[rows, :]
        outx_ref[rows, :] = moved
        xb[rows, :] = moved.astype(bf16)

    by_rows(0, width, second_move)
    gradient(2, g2)

    def second_track(rows):
        outy_ref[rows, :] = mixed(y1, y1_in, rows) + g2[rows, :] - g1[rows, :]

    def second_track_far(rows):
        second = w[2] * (y1_in[1, rows, :] + w[2] * far_in[rows, :])
        outy_ref[rows, :] = (
            w[0] * y1[rows, :] + w[1] * y1_in[0, rows, :] + second
            + g2[rows, :] - g1[rows, :]
        )

    y1_row.wait()
    on_second, others = where(second)
    for part, (start, stop) in enumerate(parts):
        for copy in y1_copies[part]:
            copy.wait()

        @on_second
        def _(part=part, start=start, stop=stop):
            for copy in (far_copies[:2], far_copies[2:])[part]:
                copy.wait_recv()
            by_rows(start, stop, second_track_far)

        @others
        def _(start=start, stop=stop):
            by_rows(start, stop, second_track)

    @on_last
    def _():
        for copy in far_copies:
            copy.wait_send()


def write_out(x_ref, y_ref, x_hbm, y_hbm, sems):
    copies = []
    for slot, (source, target) in enumerate(((x_ref, x_hbm), (y_ref, y_hbm))):
        copy = pltpu.make_async_copy(source, target, sems.at[slot])
        copy.start()
        copies.append(copy)
    for copy in copies:
        copy.wait()


def solution(mesh):
    sizes = tuple(mesh.shape[axis] for axis in AXES)

    def on_device(value_proj, token_pool, target_pool, batch_ids, frozen_out, numerators):
        width, features = value_proj.shape[2:]
        pool = token_pool.shape[2]
        rounds, batch = batch_ids.shape[2:]
        field = pltpu.VMEM((width, features), jnp.float32)
        arrivals = pltpu.VMEM((2, width, features), jnp.float32)
        in_hbm = pl.BlockSpec(memory_space=pltpu.HBM)
        shape = jax.ShapeDtypeStruct((width, features), jnp.float32)
        final_proj, final_tracker = pl.pallas_call(
            functools.partial(kernel, sizes),
            out_shape=(pltpu.VMEM((width, features), jnp.float32),) * 2,
            in_specs=[in_hbm] * 6,
            out_specs=(pl.BlockSpec(memory_space=pltpu.VMEM),) * 2,
            scratch_shapes=[
                pltpu.VMEM((pool, width), jnp.bfloat16),
                pltpu.VMEM((pool, width), jnp.bfloat16),
                pltpu.VMEM((rounds, 1, batch), jnp.int32),
                pltpu.VMEM((features, width), jnp.bfloat16),
                pltpu.SMEM(numerators.shape, jnp.int32),
                field, field, field, field, field, field,
                pltpu.VMEM((width, features), jnp.bfloat16),
                pltpu.VMEM((pool, features), jnp.bfloat16),
                arrivals, arrivals, arrivals, arrivals,
                field, field, field,
                pltpu.SemaphoreType.DMA((6,)),
                pltpu.SemaphoreType.DMA((2, 5)),
                pltpu.SemaphoreType.DMA((2, 5)),
                pltpu.SemaphoreType.DMA((3,)),
                pltpu.SemaphoreType.DMA((3,)),
                pltpu.SemaphoreType.REGULAR,
            ],
            compiler_params=pltpu.CompilerParams(
                collective_id=0, has_side_effects=True, vmem_limit_bytes=54_000_000
            ),
        )(
            value_proj.reshape(width, features),
            token_pool.reshape(pool, width),
            target_pool.reshape(pool, width),
            batch_ids.reshape(rounds, 1, batch),
            frozen_out,
            numerators,
        )
        final_proj, final_tracker = pl.pallas_call(
            write_out,
            out_shape=(shape, shape),
            in_specs=[pl.BlockSpec(memory_space=pltpu.VMEM)] * 2,
            out_specs=(in_hbm,) * 2,
            scratch_shapes=[pltpu.SemaphoreType.DMA((2,))],
            compiler_params=pltpu.CompilerParams(vmem_limit_bytes=2**20),
        )(final_proj, final_tracker)
        return final_proj[None, None], final_tracker[None, None]

    return jax.shard_map(
        on_device,
        mesh=mesh,
        in_specs=(
            P("row", "col", None, None),
            P("row", "col", None, None),
            P("row", "col", None, None),
            P("row", "col", None, None),
            P(),
            P(),
        ),
        out_specs=(P("row", "col", None, None), P("row", "col", None, None)),
        check_vma=False,
    )
```

```python
import functools
import math

import jax
import jax.numpy as jnp
from jax import lax
from jax.experimental import pallas as pl
from jax.experimental.pallas import tpu as pltpu
from jax.sharding import PartitionSpec as P

MESH = pl.DeviceIdType.MESH
step_rate = 0.2
TAIL = 64
AXES = ("row", "col")


def kernel(sizes, x0_ref, tok_hbm, tgt_hbm, ids_hbm, fo_hbm, num_hbm, outx_ref, outy_ref,
           tok, tgt, ids, fo, num_ref, x0, x1, g0, g1, g2, y1, xb, bp,
           x0_in, g0_in, x1_in, y1_in, far_in, mix2, mix3,
           local_sem, send_sem, recv_sem, far_send, far_recv, row_ready):
    pool, width = tok.shape
    features = x0.shape[1]
    factor = width ** (-0.5)
    f32, bf16 = jnp.float32, jnp.bfloat16
    early, bulk = 3 * width // 8, width - min(TAIL, width // 8)
    right, left = {}, {}
    for axis, n in zip(AXES, sizes):
        me = lax.axis_index(axis)
        right[axis], left[axis] = lax.rem(me + 1, n), lax.rem(me + n - 1, n)

    n_col = sizes[1]
    col = lax.axis_index("col")
    first, second, last = col == 0, col == 1, col == n_col - 1

    def where(condition):
        return pl.when(condition), pl.when(jnp.logical_not(condition))

    barrier = pltpu.get_barrier_semaphore()
    @pl.when(second)
    def _():
        pl.semaphore_signal(
            barrier, inc=1, device_id={"col": n_col - 1}, device_id_type=MESH
        )

    for there in ({"col": left["col"]}, {"row": right["row"]}):
        pl.semaphore_signal(barrier, inc=1, device_id=there, device_id_type=MESH)

    on_last, elsewhere = where(last)

    @on_last
    def _():
        pl.semaphore_wait(barrier, 3)

    @elsewhere
    def _():
        pl.semaphore_wait(barrier, 2)

    def describe(source, target, which, slot):
        return pltpu.make_async_remote_copy(
            src_ref=source,
            dst_ref=target,
            send_sem=send_sem.at[which, slot],
            recv_sem=recv_sem.at[which, slot],
            device_id={AXES[which]: right[AXES[which]]},
            device_id_type=MESH,
        )

    def send_rows(source, target, slot, rows, other=None):
        by_col = describe(source.at[rows], target.at[1, rows], 1, slot)
        by_row = describe(source.at[rows], target.at[0, rows], 0, slot)
        if other is None:
            by_col.start()
        else:
            @elsewhere
            def _():
                by_col.start()

            @on_last
            def _():
                describe(other.at[rows], target.at[1, rows], 1, slot).start()

        by_row.start()
        return [by_col, by_row]

    whole = pl.ds(0, width)
    x0_copies = [describe(x0_ref, x0_in.at[which], which, 0) for which in (1, 0)]
    x0_copies[0].start()
    pl.semaphore_signal(row_ready, inc=1, device_id={"row": left["row"]}, device_id_type=MESH)
    pl.semaphore_wait(row_ready, 1)
    x0_copies[1].start()

    loads = []
    for slot, (source, target) in enumerate(
        (
            (x0_ref, x0), (tok_hbm, tok), (fo_hbm, fo),
            (tgt_hbm, tgt), (ids_hbm, ids), (num_hbm, num_ref),
        )
    ):
        load = pltpu.make_async_copy(source, target, local_sem.at[slot])
        load.start()
        loads.append(load)

    step = math.gcd(width, 64)

    def by_rows(first, last, body):
        def go(i, carry):
            body(pl.ds(pl.multiple_of(i * step, step), step))
            return carry

        lax.fori_loop(first // step, last // step, go, 0)

    def mixed(own, arrived, rows):
        return w[0] * own[rows, :] + w[1] * arrived[0, rows, :] + w[2] * arrived[1, rows, :]

    block = math.gcd(pool, 256)
    wide = math.gcd(width, 256)

    def gradient(which, out):
        def forward(i, carry):
            rows = pl.ds(pl.multiple_of(i * block, block), block)
            preact = jnp.dot(tok[rows, :], xb[...], preferred_element_type=f32) * factor
            s = jax.nn.sigmoid(preact)
            hidden = (preact * s).astype(bf16)
            output = jnp.dot(hidden, fo[...], preferred_element_type=f32)
            error_term = (output - tgt[rows, :].astype(f32)).astype(bf16)
            back_hidden = lax.dot_general(
                error_term, fo[...], (((1,), (1,)), ((), ())), preferred_element_type=f32
            )
            slope = s * (1.0 + preact * (1.0 - s))
            row_ids = lax.broadcasted_iota(jnp.int32, (block, ids.shape[2]), 0) + i * block
            hits = jnp.where(row_ids == ids[which], 1.0, 0.0)
            times = jnp.sum(hits, axis=1, keepdims=True)
            bp[rows, :] = (back_hidden * slope * times).astype(bf16)
            return carry

        lax.fori_loop(0, pool // block, forward, 0)

        for j in range(width // wide):
            cols = pl.ds(j * wide, wide)
            out[cols, :] = (
                lax.dot_general(
                    tok[:, cols], bp[...], (((0,), (0,)), ((), ())), preferred_element_type=f32
                )
                * factor
            )

    for load in loads:
        load.wait()

    counts = [jnp.full((8, 128), num_ref[i], jnp.int32).astype(f32) for i in range(3)]
    total = counts[0] + counts[1] + counts[2]
    w = [(c / total)[0:1, 0:1] for c in counts]

    def first_round(rows):
        xb[rows, :] = x0[rows, :].astype(bf16)

    by_rows(0, width, first_round)
    gradient(0, g0)
    g0_col = describe(g0, g0_in.at[1], 1, 1)
    g0_row = describe(g0, g0_in.at[0], 0, 1)
    g0_row.start()

    far_copies = []
    for part, (start, stop) in enumerate(((0, early), (early, bulk), (bulk, width))):
        rows = pl.ds(start, stop - start)
        far_copies.append(
            pltpu.make_async_remote_copy(
                src_ref=g0.at[rows], dst_ref=far_in.at[rows],
                send_sem=far_send.at[part], recv_sem=far_recv.at[part],
                device_id={"col": 1}, device_id_type=MESH,
            )
        )

    @elsewhere
    def _():
        g0_col.start()

    @on_last
    def _():
        far_copies[0].start()

    for copy in x0_copies:
        copy.wait()

    def first_move(rows):
        moved = mixed(x0, x0_in, rows) - step_rate * g0[rows, :]
        x1[rows, :] = moved
        xb[rows, :] = moved.astype(bf16)

    by_rows(0, width, first_move)

    @on_last
    def _():
        def make_mix2(rows):
            mix2[rows, :] = x1[rows, :] - step_rate * g0[rows, :]

        by_rows(0, width, make_mix2)

    x1_copies = send_rows(x1, x1_in, 2, whole, mix2)
    gradient(1, g1)
    g0_row.wait()
    on_first, beyond = where(first)

    @on_first
    def _():
        def first_track(rows):
            y1[rows, :] = (
                w[0] * g0[rows, :] + w[1] * g0_in[0, rows, :] + g1[rows, :] - g0[rows, :]
            )

        by_rows(0, width, first_track)

    @beyond
    def _():
        g0_col.wait_recv()

        def first_track(rows):
            y1[rows, :] = mixed(g0, g0_in, rows) + g1[rows, :] - g0[rows, :]

        by_rows(0, width, first_track)

    @on_last
    def _():
        def make_mix3(rows):
            mix3[rows, :] = y1[rows, :] + w[0] * g0[rows, :] + w[1] * g0_in[0, rows, :]

        by_rows(0, width, make_mix3)

    parts = ((0, bulk), (bulk, width))
    y1_copies = []
    for part, (start, stop) in enumerate(parts):
        rows = pl.ds(start, stop - start)
        by_col = describe(y1.at[rows], y1_in.at[1, rows], 1, 3 + part)

        @elsewhere
        def _(by_col=by_col):
            by_col.start()

        @on_last
        def _(rows=rows, part=part):
            describe(mix3.at[rows], y1_in.at[1, rows], 1, 3 + part).start()

        y1_copies.append([by_col])
    y1_row = describe(y1, y1_in.at[0], 0, 3)
    y1_row.start()

    @elsewhere
    def _():
        g0_col.wait_send()

    @on_last
    def _():
        for copy in far_copies[1:]:
            copy.start()

    for copy in x1_copies:
        copy.wait()

    def second_move(rows):
        moved = mixed(x1, x1_in, rows) - step_rate * y1[rows, :]
        outx_ref[rows, :] = moved
        xb[rows, :] = moved.astype(bf16)

    by_rows(0, width, second_move)
    gradient(2, g2)

    def second_track(rows):
        outy_ref[rows, :] = mixed(y1, y1_in, rows) + g2[rows, :] - g1[rows, :]

    def second_track_far(rows):
        second = w[2] * (y1_in[1, rows, :] + w[2] * far_in[rows, :])
        outy_ref[rows, :] = (
            w[0] * y1[rows, :] + w[1] * y1_in[0, rows, :] + second
            + g2[rows, :] - g1[rows, :]
        )

    y1_row.wait()
    on_second, others = where(second)
    for part, (start, stop) in enumerate(parts):
        for copy in y1_copies[part]:
            copy.wait()

        @on_second
        def _(part=part, start=start, stop=stop):
            for copy in (far_copies[:2], far_copies[2:])[part]:
                copy.wait_recv()
            by_rows(start, stop, second_track_far)

        @others
        def _(start=start, stop=stop):
            by_rows(start, stop, second_track)

    @on_last
    def _():
        for copy in far_copies:
            copy.wait_send()


def write_out(x_ref, y_ref, x_hbm, y_hbm, sems):
    copies = []
    for slot, (source, target) in enumerate(((x_ref, x_hbm), (y_ref, y_hbm))):
        copy = pltpu.make_async_copy(source, target, sems.at[slot])
        copy.start()
        copies.append(copy)
    for copy in copies:
        copy.wait()


def solution(mesh):
    sizes = tuple(mesh.shape[axis] for axis in AXES)

    def on_device(value_proj, token_pool, target_pool, batch_ids, frozen_out, numerators):
        width, features = value_proj.shape[2:]
        pool = token_pool.shape[2]
        rounds, batch = batch_ids.shape[2:]
        field = pltpu.VMEM((width, features), jnp.float32)
        arrivals = pltpu.VMEM((2, width, features), jnp.float32)
        in_hbm = pl.BlockSpec(memory_space=pltpu.HBM)
        shape = jax.ShapeDtypeStruct((width, features), jnp.float32)
        final_proj, final_tracker = pl.pallas_call(
            functools.partial(kernel, sizes),
            out_shape=(pltpu.VMEM((width, features), jnp.float32),) * 2,
            in_specs=[in_hbm] * 6,
            out_specs=(pl.BlockSpec(memory_space=pltpu.VMEM),) * 2,
            scratch_shapes=[
                pltpu.VMEM((pool, width), jnp.bfloat16),
                pltpu.VMEM((pool, width), jnp.bfloat16),
                pltpu.VMEM((rounds, 1, batch), jnp.int32),
                pltpu.VMEM((features, width), jnp.bfloat16),
                pltpu.SMEM(numerators.shape, jnp.int32),
                field, field, field, field, field, field,
                pltpu.VMEM((width, features), jnp.bfloat16),
                pltpu.VMEM((pool, features), jnp.bfloat16),
                arrivals, arrivals, arrivals, arrivals,
                field, field, field,
                pltpu.SemaphoreType.DMA((6,)),
                pltpu.SemaphoreType.DMA((2, 5)),
                pltpu.SemaphoreType.DMA((2, 5)),
                pltpu.SemaphoreType.DMA((3,)),
                pltpu.SemaphoreType.DMA((3,)),
                pltpu.SemaphoreType.REGULAR,
            ],
            compiler_params=pltpu.CompilerParams(
                collective_id=0, has_side_effects=True, vmem_limit_bytes=54_000_000
            ),
        )(
            value_proj.reshape(width, features),
            token_pool.reshape(pool, width),
            target_pool.reshape(pool, width),
            batch_ids.reshape(rounds, 1, batch),
            frozen_out,
            numerators,
        )
        final_proj, final_tracker = pl.pallas_call(
            write_out,
            out_shape=(shape, shape),
            in_specs=[pl.BlockSpec(memory_space=pltpu.VMEM)] * 2,
            out_specs=(in_hbm,) * 2,
            scratch_shapes=[pltpu.SemaphoreType.DMA((2,))],
            compiler_params=pltpu.CompilerParams(vmem_limit_bytes=2**20),
        )(final_proj, final_tracker)
        return final_proj[None, None], final_tracker[None, None]

    return jax.shard_map(
        on_device,
        mesh=mesh,
        in_specs=(
            P("row", "col", None, None),
            P("row", "col", None, None),
            P("row", "col", None, None),
            P("row", "col", None, None),
            P(),
            P(),
        ),
        out_specs=(P("row", "col", None, None), P("row", "col", None, None)),
        check_vma=False,
    )
```
